256 devices in a mesh: zero: 32 (over z_0, y, x), width: 2 (over z_1), site: 4 (over z_2, core).
Axes of the slice: x: 4, y: 4, z: 8 (z_0: 2, z_1: 2, z_2: 2; z = z_0 * 4 + z_1 * 2 + z_2), core: 2. Of those that a mesh axis runs over, the one named last changes fastest.
Arguments:
- train_query: bfloat16 [28672, 7168], P(('site', 'zero'), 'width'), parts along dimension 0, may hold values from -0.125 to 0.125
- low_query: bfloat16 [28672, 64], P(('site', 'zero')), parts along dimension 0, may hold values from -0.0625 to 0.0625
- high_query: bfloat16 [256, 7168], P('site', 'width'), parts along dimension 0, may hold values from -0.75 to 0.75
- train_key: bfloat16 [28672, 7168], P(('site', 'zero'), 'width'), parts along dimension 0, may hold values from -0.125 to 0.125
- low_key: bfloat16 [28672, 64], P(('site', 'zero')), parts along dimension 0, may hold values from -0.0625 to 0.0625
- high_key: bfloat16 [256, 7168], P('site', 'width'), parts along dimension 0, may hold values from -0.75 to 0.75
- train_value: bfloat16 [28672, 7168], P(('site', 'zero'), 'width'), parts along dimension 0, may hold values from -0.125 to 0.125
- low_value: bfloat16 [28672, 64], P(('site', 'zero')), parts along dimension 0, may hold values from -0.0625 to 0.0625
- high_value: bfloat16 [256, 7168], P('site', 'width'), parts along dimension 0, may hold values from -0.75 to 0.75
- norm_train: float32 [28672], P(('site', 'zero', 'width')), parts along dimension 0, may hold values from 0.25 to 1.75
- norm_step: float32 [28672], P(('site', 'zero', 'width')), parts along dimension 0, may hold values from -0.3 to 0.3
Outputs:
- final_query: bfloat16 [28672, 7168], P('site', ('width', 'zero')), parts along dimension 0
- final_key: bfloat16 [28672, 7168], P('site', ('width', 'zero')), parts along dimension 0
- final_value: bfloat16 [28672, 7168], P('site', ('width', 'zero')), parts along dimension 0
- scale_query: float32 [28672], P(('site', 'width', 'zero')), parts along dimension 0
- scale_key: float32 [28672], P(('site', 'width', 'zero')), parts along dimension 0
- scale_value: float32 [28672], P(('site', 'width', 'zero')), parts along dimension 0
- serve_norm: bfloat16 [28672], P('site'), parts along dimension 0
The draws below stay inside these ranges and needn't reach their ends.
There are 4 independent parts, one for each index of `site`. The reference program is written for one: setup_inputs(seed, part) draws one part's arguments, and reference() takes and returns one part's arrays. A program takes and returns all parts, laid end to end along the dimension named above; each array names one. Nothing has to cross between parts.
All inputs are finite; a program needn't handle non-finite values. Where the reference program divides by a largest or mean magnitude, that divisor is 1e-20 or more.
Results may differ from the reference program's by a relative error of at most 0.01.
Values may be sent and summed in bfloat16 or wider, within the bound.
A program may use at most 128 MiB of HBM per device.

```python
import jax
import jax.numpy as jnp

D_MODEL = 7168
Q_DIM = 7168
KV_DIM = 7168
RANK = 64


def with_spikes(values, own_key, source, target, shards_of, factor):
    owner, partner = [(jnp.arange(values.shape[position]) // (values.shape[position] // shards_of)).reshape([-1 if axis == position else 1 for axis in range(values.ndim)]) for position in (source, target)]
    chosen = jax.random.permutation(own_key, shards_of)[partner]
    strong = (owner == chosen) | (owner == (partner + shards_of // 2) % shards_of)
    return jnp.where(strong, factor * values, values)


def block_levels(rng, extent, pieces, smallest, high):
    loudness = 1.0
    for position, parts in pieces:
        heights = jax.random.uniform(jax.random.fold_in(jax.random.fold_in(rng, 6), position), (parts,), jnp.float32, smallest / len(pieces), high / len(pieces))
        loudness = loudness * jnp.repeat(jnp.exp(heights), extent[position] // parts).reshape((-1,) + (1,) * (len(extent) - 1 - position))
    return loudness


def scatter_about(key, extent, scale, most, pieces=(), dtype=jnp.bfloat16):
    loudness = block_levels(key, extent, pieces, -0.22, 0.18) if pieces else 1.0
    values = jax.random.normal(key, extent, jnp.float32) * scale * loudness
    return jnp.minimum(jnp.maximum(values, -most), most).astype(dtype)


def gaussian_with(own_key, shape, width, reach, shards, heavy, held_as=jnp.bfloat16):
    array = width * jax.random.normal(own_key, shape, jnp.float32)
    if shards:
        array = array * block_levels(own_key, shape, shards, -0.22, 0.18)
    return jnp.clip(with_spikes(array, jax.random.fold_in(own_key, 3), *heavy), -reach, reach).astype(held_as)


def setup_inputs(seed: int = 0, part: int = 0) -> dict:
    key_list = jax.random.split(jax.random.key(seed), 12)
    own_keys = jax.random.split(jax.random.fold_in(key_list[11], part), 12)
    train_query = gaussian_with(own_keys[0], (D_MODEL, Q_DIM), D_MODEL ** -0.5, 0.125, ((0, 32), (1, 2)), (0, 1, 32, 2.75))
    low_query = scatter_about(own_keys[1], (D_MODEL, RANK), D_MODEL ** -0.5, 0.0625, ((0, 32),))
    high_query = scatter_about(own_keys[2], (RANK, Q_DIM), RANK ** -0.5, 0.75, ((1, 2),))
    train_key = gaussian_with(own_keys[3], (D_MODEL, KV_DIM), D_MODEL ** -0.5, 0.125, ((0, 32), (1, 2)), (0, 1, 32, 2.75))
    low_key = scatter_about(own_keys[4], (D_MODEL, RANK), D_MODEL ** -0.5, 0.0625, ((0, 32),))
    high_key = scatter_about(own_keys[5], (RANK, KV_DIM), RANK ** -0.5, 0.75, ((1, 2),))
    train_value = gaussian_with(own_keys[6], (D_MODEL, KV_DIM), D_MODEL ** -0.5, 0.125, ((0, 32), (1, 2)), (0, 1, 32, 2.75))
    low_value = scatter_about(own_keys[7], (D_MODEL, RANK), D_MODEL ** -0.5, 0.0625, ((0, 32),))
    high_value = scatter_about(own_keys[8], (RANK, KV_DIM), RANK ** -0.5, 0.75, ((1, 2),))
    norm_train = jnp.clip(1.0 + 0.15 * jax.random.normal(own_keys[9], (D_MODEL,), jnp.float32), 0.25, 1.75)
    norm_step = jnp.clip(jax.random.uniform(own_keys[10], (D_MODEL,), jnp.float32, -0.3, 0.3) * block_levels(own_keys[10], (D_MODEL,), ((0, 64),), -0.4, 0.0), -0.3, 0.3)
    return dict(train_query=train_query, low_query=low_query, high_query=high_query, train_key=train_key, low_key=low_key, high_key=high_key, train_value=train_value, low_value=low_value, high_value=high_value, norm_train=norm_train, norm_step=norm_step)


mix_rate = 1.0


def reference(train_query, low_query, high_query, train_key, low_key, high_key, train_value, low_value, high_value, norm_train, norm_step):
    result_query = train_query.astype(jnp.float32) + mix_rate * jnp.dot(low_query, high_query, preferred_element_type=jnp.float32)
    result_key = train_key.astype(jnp.float32) + mix_rate * jnp.dot(low_key, high_key, preferred_element_type=jnp.float32)
    result_value = train_value.astype(jnp.float32) + mix_rate * jnp.dot(low_value, high_value, preferred_element_type=jnp.float32)
    scale_query = jnp.sum(jnp.abs(result_query), axis=0) / D_MODEL
    final_query = (result_query / scale_query).astype(jnp.bfloat16)
    scale_key = jnp.sum(jnp.abs(result_key), axis=0) / D_MODEL
    final_key = (result_key / scale_key).astype(jnp.bfloat16)
    scale_value = jnp.sum(jnp.abs(result_value), axis=0) / D_MODEL
    final_value = (result_value / scale_value).astype(jnp.bfloat16)
    serve_norm = (norm_train + norm_step).astype(jnp.bfloat16)
    return final_query, final_key, final_value, scale_query, scale_key, scale_value, serve_norm
```

```python
import functools

import jax
import jax.numpy as jnp
from jax import lax
from jax.experimental import pallas as pl
from jax.experimental.pallas import tpu as pltpu
from jax.sharding import PartitionSpec as P

D_MODEL = 7168
MIX_RATE = 1.0
ROWS = 224
COLS = 3584
OWN = 112
RANK = 64
PEERS = 32
HALF = PEERS // 2
BLOCK = 200
BASE = 88
SPILL = OWN - BASE
MESH = pl.DeviceIdType.MESH
VMEM_LIMIT = 56 << 20


def unit_of_lane(rows):
    return lax.broadcasted_iota(jnp.int32, (rows, 128), 1) // 32


def packed(block, free):
    first, tail = block[:, :128], block[:, 128:]
    spill = tail[BASE:]
    moved = jnp.concatenate(
        [pltpu.roll(spill, 128 - 32 * i, axis=1) for i in (1, 2, 3)], axis=0
    )
    holds = 3 * SPILL
    mixed = jnp.where(unit_of_lane(holds) == free, moved, tail[:holds])
    return jnp.concatenate([first, mixed, tail[holds:BASE]], axis=0)


def unpacked(block, free):
    first, base = block[:OWN], block[OWN:]
    unit = unit_of_lane(SPILL)
    spill = jnp.zeros((SPILL, 128), jnp.float32)
    for i in (1, 2, 3):
        piece = pltpu.roll(base[SPILL * (i - 1) : SPILL * i], 32 * i, axis=1)
        spill = jnp.where(unit == (free + i) % 4, piece, spill)
    return first, jnp.concatenate([base, spill], axis=0)


def gather_columns(received, sums, joined, groups):
    lane = lax.broadcasted_iota(jnp.int32, (OWN, 128), 1)

    def step(i, total):
        group = groups(i)
        at = pl.multiple_of(group * 896, 128)
        parts = [
            unpacked(received[group * 4 + b].astype(jnp.float32), 3 - b) for b in range(4)
        ]
        tiles = []
        for b in range(4):
            tiles.append(parts[b][0])
            if b < 3:
                tiles.append(jnp.where(lane < 96 - 32 * b, parts[b][1], parts[b + 1][1]))
        for t, tile in enumerate(tiles):
            joined[:, pl.ds(at + 128 * t, 128)] = tile.astype(jnp.bfloat16)
            total = total + jnp.abs(tile)
        return total

    sums[...] = lax.fori_loop(0, 4, step, sums[...])


def scaled(joined, sums, final):
    scale = jnp.sum(sums[...], axis=1, keepdims=True) / D_MODEL
    factor = jnp.broadcast_to(1.0 / scale, (OWN, 896))

    def step(i, carry):
        at = pl.multiple_of(i * 896, 128)
        part = joined[:, pl.ds(at, 896)].astype(jnp.float32) * factor
        final[:, pl.ds(at, 896)] = part.astype(jnp.bfloat16)
        return carry

    lax.fori_loop(0, 8, step, 0)


def as_row(sums):
    scale = jnp.broadcast_to(
        jnp.sum(sums[...], axis=1, keepdims=True) / D_MODEL, (OWN, OWN)
    )
    row = lax.broadcasted_iota(jnp.int32, (OWN, OWN), 0)
    column = lax.broadcasted_iota(jnp.int32, (OWN, OWN), 1)
    return jnp.sum(jnp.where(row == column, scale, 0.0), axis=0, keepdims=True)


def exchange(
    train_q, low_q, high_q, train_k, low_k, high_k, train_v, low_v, high_v, norm, step,
    joined_q, joined_k, joined_v, sums_q, sums_k, sums_v, gains,
    train, low, high, result, outgoing, received,
    load_sem, send_sem, recv_sem, gain_send, gain_recv, pair_send, pair_recv,
):
    me = lax.axis_index("zero")
    width = lax.axis_index("width")
    site = lax.axis_index("site")
    far, y, x = me // 16, (me // 4) % 4, me % 4
    turn = me % 4
    sources = ((train_q, low_q, high_q), (train_k, low_k, high_k), (train_v, low_v, high_v))

    loads = []
    for m, refs in enumerate(sources):
        for part, (ref, buffer) in enumerate(zip(refs, (train, low, high), strict=True)):
            loads.append(pltpu.make_async_copy(ref, buffer.at[m], load_sem.at[m, part]))
            loads[-1].start()

    barrier = pltpu.get_barrier_semaphore()

    def greet(i, carry):
        peer = (me + i) % PEERS
        pl.semaphore_signal(barrier, inc=1, device_id=(peer, width, site), device_id_type=MESH)
        return carry

    lax.fori_loop(1, PEERS, greet, 0)
    partner = (me, 1 - width, site)
    pl.semaphore_signal(barrier, inc=1, device_id=partner, device_id_type=MESH)

    gain = (norm[...] + step[...]).astype(jnp.bfloat16).astype(jnp.float32)
    gains[me, pl.ds(width, 1), :] = jnp.concatenate(
        [gain, jnp.zeros((1, 128 - OWN), jnp.float32)], axis=1
    )

    from_row = lax.broadcasted_iota(jnp.int32, (ROWS, 256), 0)
    to_lane = lax.broadcasted_iota(jnp.int32, (ROWS, 256), 1)
    place = jnp.where(from_row == (to_lane + 32 * turn) % 256, 1.0, 0.0).astype(jnp.bfloat16)

    def merge(m, half):
        base = half * (COLS // 2)
        turned_low = jnp.dot(low[m], place, preferred_element_type=jnp.float32).astype(
            jnp.bfloat16
        )

        def columns(c, carry):
            at = pl.multiple_of(base + c * 256, 128)
            dims = (((0,), (0,)), ((), ()))
            part = lax.dot_general(
                train[m, :, pl.ds(at, 256)], place, dims, preferred_element_type=jnp.float32
            )
            part = part + MIX_RATE * lax.dot_general(
                high[m, :, pl.ds(at, 256)], turned_low, dims, preferred_element_type=jnp.float32
            )
            result[pl.ds(pl.multiple_of(c * 256, 256), 256), :] = part
            return carry

        lax.fori_loop(0, COLS // 512, columns, 0)

        def block(j, carry):
            part = result[pl.ds(pl.multiple_of(j * OWN, 8), OWN), :]
            outgoing[m, half * HALF + j] = packed(part, 3 - turn).astype(jnp.bfloat16)
            return carry

        lax.fori_loop(0, HALF, block, 0)

    def send(m, peer, sem):
        pltpu.make_async_remote_copy(
            src_ref=outgoing.at[m, peer],
            dst_ref=received.at[m, me],
            send_sem=send_sem.at[m],
            recv_sem=recv_sem.at[m, sem],
            device_id=(peer, width, site),
            device_id_type=MESH,
        ).start()

    def relative(half, i):
        return half * HALF + ((y + i // 4) % 4) * 4 + (x + i % 4) % 4

    for m in range(3):
        for part in range(3):
            loads[3 * m + part].wait()
        merge(m, 1 - far)
        if m == 0:
            pl.semaphore_wait(barrier, PEERS)
            pltpu.make_async_remote_copy(
                src_ref=gains.at[me, pl.ds(width, 1)],
                dst_ref=gains.at[me, pl.ds(width, 1)],
                send_sem=pair_send,
                recv_sem=pair_recv,
                device_id=partner,
                device_id_type=MESH,
            ).start()

        def over(i, carry, m=m):
            send(m, relative(1 - far, i), 0)
            return carry

        lax.fori_loop(0, HALF, over, 0)
        merge(m, far)

        def near(i, carry, m=m):
            send(m, relative(far, i), 1)
            return carry

        lax.fori_loop(1, HALF, near, 0)
        received[m, me] = outgoing[m, me]

    pair = pltpu.make_async_remote_copy(
        src_ref=gains.at[me, pl.ds(width, 1)],
        dst_ref=gains.at[me, pl.ds(1 - width, 1)],
        send_sem=pair_send,
        recv_sem=pair_recv,
        device_id=partner,
        device_id_type=MESH,
    )
    pair.wait_recv()

    def spread(i, carry):
        pltpu.make_async_remote_copy(
            src_ref=gains.at[me],
            dst_ref=gains.at[me],
            send_sem=gain_send,
            recv_sem=gain_recv,
            device_id=((me + i) % PEERS, width, site),
            device_id_type=MESH,
        ).start()
        return carry

    lax.fori_loop(1, PEERS, spread, 0)

    def arrived(m, sem, blocks):
        window = received.at[m, pl.ds(0, blocks)]
        pltpu.make_async_copy(window, window, recv_sem.at[m, sem]).wait()

    for m, (joined, sums) in enumerate(
        ((joined_q, sums_q), (joined_k, sums_k), (joined_v, sums_v))
    ):
        sums[...] = jnp.zeros_like(sums)
        arrived(m, 1, HALF - 1)
        gather_columns(received.at[m], sums, joined, lambda i: far * 4 + i)
        arrived(m, 0, HALF)
        gather_columns(received.at[m], sums, joined, lambda i: (1 - far) * 4 + i)
        if m < 2:
            scaled(joined, sums, joined)

    rest = gains.at[pl.ds(0, PEERS - 1)]
    pltpu.make_async_copy(rest, rest, gain_recv).wait()
    pltpu.make_async_copy(rest, rest, gain_send).wait()
    pair.wait_send()
    for m in range(3):
        window = outgoing.at[m, pl.ds(0, PEERS - 1)]
        pltpu.make_async_copy(window, window, send_sem.at[m]).wait()


def finish(
    joined_q, joined_k, joined_v, sums_q, sums_k, sums_v, gains,
    final_q, final_k, final_v, scale_q, scale_k, scale_v, serve,
    last, rows, sem,
):
    copies = [
        pltpu.make_async_copy(joined_q, final_q, sem.at[0]),
        pltpu.make_async_copy(joined_k, final_k, sem.at[1]),
        pltpu.make_async_copy(last, final_v, sem.at[2]),
    ]
    copies[0].start()
    copies[1].start()
    scaled(joined_v, sums_v, last)
    copies[2].start()
    for sums, scale in ((sums_q, scale_q), (sums_k, scale_k), (sums_v, scale_v)):
        scale[...] = as_row(sums)
    lane = lax.broadcasted_iota(jnp.int32, (1, 128), 1)
    for r in range(D_MODEL // 128):
        group, place = r // 7 * 8, r % 7
        left = gains[pl.ds(group + place, 1), :]
        right = gains[pl.ds(group + place + 1, 1), :]
        if place:
            left = pltpu.roll(left, 128 - 16 * place, axis=1)
        right = pltpu.roll(right, OWN - 16 * place, axis=1)
        rows[pl.ds(r, 1), :] = jnp.where(lane < OWN - 16 * place, left, right)
    serve[...] = rows[...].astype(jnp.bfloat16)
    for copy in copies:
        copy.wait()


def shards(
    train_query, low_query, high_query,
    train_key, low_key, high_key,
    train_value, low_value, high_value,
    norm_train, norm_step,
):
    anywhere = pl.BlockSpec(memory_space=pl.ANY)
    vmem = pl.BlockSpec(memory_space=pltpu.VMEM)
    whole = jax.ShapeDtypeStruct((OWN, D_MODEL), jnp.bfloat16)
    lanes = jax.ShapeDtypeStruct((OWN, 128), jnp.float32)
    dma = pltpu.SemaphoreType.DMA
    *middle, gains = pl.pallas_call(
        exchange,
        name="exchange",
        out_shape=(
            *[whole] * 3, *[lanes] * 3, jax.ShapeDtypeStruct((PEERS, 2, 128), jnp.float32),
        ),
        in_specs=[anywhere] * 9 + [vmem] * 2,
        out_specs=(vmem,) * 7,
        scratch_shapes=[
            pltpu.VMEM((3, ROWS, COLS), jnp.bfloat16),
            pltpu.VMEM((3, RANK, ROWS), jnp.bfloat16),
            pltpu.VMEM((3, RANK, COLS), jnp.bfloat16),
            pltpu.VMEM((COLS // 2, 256), jnp.float32),
            pltpu.VMEM((3, PEERS, BLOCK, 128), jnp.bfloat16),
            pltpu.VMEM((3, PEERS, BLOCK, 128), jnp.bfloat16),
            dma((3, 3)), dma((3,)), dma((3, 2)), dma, dma, dma, dma,
        ],
        compiler_params=pltpu.CompilerParams(
            collective_id=0, has_side_effects=True, vmem_limit_bytes=VMEM_LIMIT
        ),
    )(
        train_query, low_query.T, high_query,
        train_key, low_key.T, high_key,
        train_value, low_value.T, high_value,
        norm_train.reshape(1, OWN), norm_step.reshape(1, OWN),
    )
    *finals, scale_q, scale_k, scale_v, serve = pl.pallas_call(
        finish,
        name="finish",
        out_shape=(
            *[whole] * 3,
            *[jax.ShapeDtypeStruct((1, OWN), jnp.float32)] * 3,
            jax.ShapeDtypeStruct((D_MODEL // 128, 128), jnp.bfloat16),
        ),
        in_specs=[vmem] * 7,
        out_specs=(anywhere,) * 3 + (vmem,) * 4,
        scratch_shapes=[
            pltpu.VMEM((OWN, D_MODEL), jnp.bfloat16),
            pltpu.VMEM((D_MODEL // 128, 128), jnp.float32),
            dma((3,)),
        ],
        compiler_params=pltpu.CompilerParams(vmem_limit_bytes=16 << 20),
    )(*middle, gains.reshape(2 * PEERS, 128))
    return (
        *[final.T for final in finals],
        scale_q.reshape(OWN), scale_k.reshape(OWN), scale_v.reshape(OWN),
        serve.reshape(D_MODEL),
    )


def solution(mesh):
    weights = (P(("site", "zero"), "width"), P(("site", "zero"), None), P("site", "width"))
    gain = P(("site", "zero", "width"))
    return jax.shard_map(
        shards,
        mesh=mesh,
        in_specs=weights * 3 + (gain, gain),
        out_specs=(P("site", ("width", "zero")),) * 3
        + (P(("site", "width", "zero")),) * 3
        + (P("site"),),
        check_vma=False,
    )
```

```python
import functools

import jax
import jax.numpy as jnp
from jax import lax
from jax.experimental import pallas as pl
from jax.experimental.pallas import tpu as pltpu
from jax.sharding import PartitionSpec as P

D_MODEL = 7168
MIX_RATE = 1.0
ROWS = 224
COLS = 3584
OWN = 112
RANK = 64
PEERS = 32
HALF = PEERS // 2
BLOCK = 200
BASE = 88
SPILL = OWN - BASE
MESH = pl.DeviceIdType.MESH
VMEM_LIMIT = 56 << 20


def unit_of_lane(rows):
    return lax.broadcasted_iota(jnp.int32, (rows, 128), 1) // 32


def packed(block, free):
    first, tail = block[:, :128], block[:, 128:]
    spill = tail[BASE:]
    moved = jnp.concatenate(
        [pltpu.roll(spill, 128 - 32 * i, axis=1) for i in (1, 2, 3)], axis=0
    )
    holds = 3 * SPILL
    mixed = jnp.where(unit_of_lane(holds) == free, moved, tail[:holds])
    return jnp.concatenate([first, mixed, tail[holds:BASE]], axis=0)


def unpacked(block, free):
    first, base = block[:OWN], block[OWN:]
    unit = unit_of_lane(SPILL)
    spill = jnp.zeros((SPILL, 128), jnp.float32)
    for i in (1, 2, 3):
        piece = pltpu.roll(base[SPILL * (i - 1) : SPILL * i], 32 * i, axis=1)
        spill = jnp.where(unit == (free + i) % 4, piece, spill)
    return first, jnp.concatenate([base, spill], axis=0)


def gather_columns(received, sums, joined, groups):
    lane = lax.broadcasted_iota(jnp.int32, (OWN, 128), 1)

    def step(i, total):
        group = groups(i)
        at = pl.multiple_of(group * 896, 128)
        parts = [
            unpacked(received[group * 4 + b].astype(jnp.float32), 3 - b) for b in range(4)
        ]
        tiles = []
        for b in range(4):
            tiles.append(parts[b][0])
            if b < 3:
                tiles.append(jnp.where(lane < 96 - 32 * b, parts[b][1], parts[b + 1][1]))
        for t, tile in enumerate(tiles):
            joined[:, pl.ds(at + 128 * t, 128)] = tile.astype(jnp.bfloat16)
            total = total + jnp.abs(tile)
        return total

    sums[...] = lax.fori_loop(0, 4, step, sums[...])


def scaled(joined, sums, final):
    scale = jnp.sum(sums[...], axis=1, keepdims=True) / D_MODEL
    factor = jnp.broadcast_to(1.0 / scale, (OWN, 896))

    def step(i, carry):
        at = pl.multiple_of(i * 896, 128)
        part = joined[:, pl.ds(at, 896)].astype(jnp.float32) * factor
        final[:, pl.ds(at, 896)] = part.astype(jnp.bfloat16)
        return carry

    lax.fori_loop(0, 8, step, 0)


def as_row(sums):
    scale = jnp.broadcast_to(
        jnp.sum(sums[...], axis=1, keepdims=True) / D_MODEL, (OWN, OWN)
    )
    row = lax.broadcasted_iota(jnp.int32, (OWN, OWN), 0)
    column = lax.broadcasted_iota(jnp.int32, (OWN, OWN), 1)
    return jnp.sum(jnp.where(row == column, scale, 0.0), axis=0, keepdims=True)


def exchange(
    train_q, low_q, high_q, train_k, low_k, high_k, train_v, low_v, high_v, norm, step,
    joined_q, joined_k, joined_v, sums_q, sums_k, sums_v, gains,
    train, low, high, result, outgoing, received,
    load_sem, send_sem, recv_sem, gain_send, gain_recv, pair_send, pair_recv,
):
    me = lax.axis_index("zero")
    width = lax.axis_index("width")
    site = lax.axis_index("site")
    far, y, x = me // 16, (me // 4) % 4, me % 4
    turn = me % 4
    sources = ((train_q, low_q, high_q), (train_k, low_k, high_k), (train_v, low_v, high_v))

    loads = []
    for m, refs in enumerate(sources):
        for part, (ref, buffer) in enumerate(zip(refs, (train, low, high), strict=True)):
            loads.append(pltpu.make_async_copy(ref, buffer.at[m], load_sem.at[m, part]))
            loads[-1].start()

    barrier = pltpu.get_barrier_semaphore()

    def greet(i, carry):
        peer = (me + i) % PEERS
        pl.semaphore_signal(barrier, inc=1, device_id=(peer, width, site), device_id_type=MESH)
        return carry

    lax.fori_loop(1, PEERS, greet, 0)
    partner = (me, 1 - width, site)
    pl.semaphore_signal(barrier, inc=1, device_id=partner, device_id_type=MESH)

    gain = (norm[...] + step[...]).astype(jnp.bfloat16).astype(jnp.float32)
    gains[me, pl.ds(width, 1), :] = jnp.concatenate(
        [gain, jnp.zeros((1, 128 - OWN), jnp.float32)], axis=1
    )

    from_row = lax.broadcasted_iota(jnp.int32, (ROWS, 256), 0)
    to_lane = lax.broadcasted_iota(jnp.int32, (ROWS, 256), 1)
    place = jnp.where(from_row == (to_lane + 32 * turn) % 256, 1.0, 0.0).astype(jnp.bfloat16)

    def merge(m, half):
        base = half * (COLS // 2)
        turned_low = jnp.dot(low[m], place, preferred_element_type=jnp.float32).astype(
            jnp.bfloat16
        )

        def columns(c, carry):
            at = pl.multiple_of(base + c * 256, 128)
            dims = (((0,), (0,)), ((), ()))
            part = lax.dot_general(
                train[m, :, pl.ds(at, 256)], place, dims, preferred_element_type=jnp.float32
            )
            part = part + MIX_RATE * lax.dot_general(
                high[m, :, pl.ds(at, 256)], turned_low, dims, preferred_element_type=jnp.float32
            )
            result[pl.ds(pl.multiple_of(c * 256, 256), 256), :] = part
            return carry

        lax.fori_loop(0, COLS // 512, columns, 0)

        def block(j, carry):
            part = result[pl.ds(pl.multiple_of(j * OWN, 8), OWN), :]
            outgoing[m, half * HALF + j] = packed(part, 3 - turn).astype(jnp.bfloat16)
            return carry

        lax.fori_loop(0, HALF, block, 0)

    def send(m, peer, sem):
        pltpu.make_async_remote_copy(
            src_ref=outgoing.at[m, peer],
            dst_ref=received.at[m, me],
            send_sem=send_sem.at[m],
            recv_sem=recv_sem.at[m, sem],
            device_id=(peer, width, site),
            device_id_type=MESH,
        ).start()

    def relative(half, i):
        return half * HALF + ((y + i // 4) % 4) * 4 + (x + i % 4) % 4

    for m in range(3):
        for part in range(3):
            loads[3 * m + part].wait()
        merge(m, 1 - far)
        if m == 0:
            pl.semaphore_wait(barrier, PEERS)
            pltpu.make_async_remote_copy(
                src_ref=gains.at[me, pl.ds(width, 1)],
                dst_ref=gains.at[me, pl.ds(width, 1)],
                send_sem=pair_send,
                recv_sem=pair_recv,
                device_id=partner,
                device_id_type=MESH,
            ).start()

        def over(i, carry, m=m):
            send(m, relative(1 - far, i), 0)
            return carry

        lax.fori_loop(0, HALF, over, 0)
        merge(m, far)

        def near(i, carry, m=m):
            send(m, relative(far, i), 1)
            return carry

        lax.fori_loop(1, HALF, near, 0)
        received[m, me] = outgoing[m, me]

    pair = pltpu.make_async_remote_copy(
        src_ref=gains.at[me, pl.ds(width, 1)],
        dst_ref=gains.at[me, pl.ds(1 - width, 1)],
        send_sem=pair_send,
        recv_sem=pair_recv,
        device_id=partner,
        device_id_type=MESH,
    )
    pair.wait_recv()

    def spread(i, carry):
        pltpu.make_async_remote_copy(
            src_ref=gains.at[me],
            dst_ref=gains.at[me],
            send_sem=gain_send,
            recv_sem=gain_recv,
            device_id=((me + i) % PEERS, width, site),
            device_id_type=MESH,
        ).start()
        return carry

    lax.fori_loop(1, PEERS, spread, 0)

    def arrived(m, sem, blocks):
        window = received.at[m, pl.ds(0, blocks)]
        pltpu.make_async_copy(window, window, recv_sem.at[m, sem]).wait()

    for m, (joined, sums) in enumerate(
        ((joined_q, sums_q), (joined_k, sums_k), (joined_v, sums_v))
    ):
        sums[...] = jnp.zeros_like(sums)
        arrived(m, 1, HALF - 1)
        gather_columns(received.at[m], sums, joined, lambda i: far * 4 + i)
        arrived(m, 0, HALF)
        gather_columns(received.at[m], sums, joined, lambda i: (1 - far) * 4 + i)
        if m < 2:
            scaled(joined, sums, joined)

    rest = gains.at[pl.ds(0, PEERS - 1)]
    pltpu.make_async_copy(rest, rest, gain_recv).wait()
    pltpu.make_async_copy(rest, rest, gain_send).wait()
    pair.wait_send()
    for m in range(3):
        window = outgoing.at[m, pl.ds(0, PEERS - 1)]
        pltpu.make_async_copy(window, window, send_sem.at[m]).wait()


def finish(
    joined_q, joined_k, joined_v, sums_q, sums_k, sums_v, gains,
    final_q, final_k, final_v, scale_q, scale_k, scale_v, serve,
    last, rows, sem,
):
    copies = [
        pltpu.make_async_copy(joined_q, final_q, sem.at[0]),
        pltpu.make_async_copy(joined_k, final_k, sem.at[1]),
        pltpu.make_async_copy(last, final_v, sem.at[2]),
    ]
    copies[0].start()
    copies[1].start()
    scaled(joined_v, sums_v, last)
    copies[2].start()
    for sums, scale in ((sums_q, scale_q), (sums_k, scale_k), (sums_v, scale_v)):
        scale[...] = as_row(sums)
    lane = lax.broadcasted_iota(jnp.int32, (1, 128), 1)
    for r in range(D_MODEL // 128):
        group, place = r // 7 * 8, r % 7
        left = gains[pl.ds(group + place, 1), :]
        right = gains[pl.ds(group + place + 1, 1), :]
        if place:
            left = pltpu.roll(left, 128 - 16 * place, axis=1)
        right = pltpu.roll(right, OWN - 16 * place, axis=1)
        rows[pl.ds(r, 1), :] = jnp.where(lane < OWN - 16 * place, left, right)
    serve[...] = rows[...].astype(jnp.bfloat16)
    for copy in copies:
        copy.wait()


def shards(
    train_query, low_query, high_query,
    train_key, low_key, high_key,
    train_value, low_value, high_value,
    norm_train, norm_step,
):
    anywhere = pl.BlockSpec(memory_space=pl.ANY)
    vmem = pl.BlockSpec(memory_space=pltpu.VMEM)
    whole = jax.ShapeDtypeStruct((OWN, D_MODEL), jnp.bfloat16)
    held = pltpu.VMEM((OWN, D_MODEL), jnp.bfloat16)
    lanes = pltpu.VMEM((OWN, 128), jnp.float32)
    dma = pltpu.SemaphoreType.DMA
    *middle, gains = pl.pallas_call(
        exchange,
        name="exchange",
        out_shape=(
            *[held] * 3, *[lanes] * 3, pltpu.VMEM((PEERS, 2, 128), jnp.float32),
        ),
        in_specs=[anywhere] * 9 + [vmem] * 2,
        out_specs=(vmem,) * 7,
        scratch_shapes=[
            pltpu.VMEM((3, ROWS, COLS), jnp.bfloat16),
            pltpu.VMEM((3, RANK, ROWS), jnp.bfloat16),
            pltpu.VMEM((3, RANK, COLS), jnp.bfloat16),
            pltpu.VMEM((COLS // 2, 256), jnp.float32),
            pltpu.VMEM((3, PEERS, BLOCK, 128), jnp.bfloat16),
            pltpu.VMEM((3, PEERS, BLOCK, 128), jnp.bfloat16),
            dma((3, 3)), dma((3,)), dma((3, 2)), dma, dma, dma, dma,
        ],
        compiler_params=pltpu.CompilerParams(
            collective_id=0, has_side_effects=True, vmem_limit_bytes=VMEM_LIMIT
        ),
    )(
        train_query, low_query.T, high_query,
        train_key, low_key.T, high_key,
        train_value, low_value.T, high_value,
        norm_train.reshape(1, OWN), norm_step.reshape(1, OWN),
    )
    *finals, scale_q, scale_k, scale_v, serve = pl.pallas_call(
        finish,
        name="finish",
        out_shape=(
            *[whole] * 3,
            *[jax.ShapeDtypeStruct((1, OWN), jnp.float32)] * 3,
            jax.ShapeDtypeStruct((D_MODEL // 128, 128), jnp.bfloat16),
        ),
        in_specs=[vmem] * 7,
        out_specs=(anywhere,) * 3 + (vmem,) * 4,
        scratch_shapes=[
            pltpu.VMEM((OWN, D_MODEL), jnp.bfloat16),
            pltpu.VMEM((D_MODEL // 128, 128), jnp.float32),
            dma((3,)),
        ],
        compiler_params=pltpu.CompilerParams(vmem_limit_bytes=16 << 20),
    )(*middle, gains.reshape(2 * PEERS, 128))
    return (
        *[final.T for final in finals],
        scale_q.reshape(OWN), scale_k.reshape(OWN), scale_v.reshape(OWN),
        serve.reshape(D_MODEL),
    )


def solution(mesh):
    weights = (P(("site", "zero"), "width"), P(("site", "zero"), None), P("site", "width"))
    gain = P(("site", "zero", "width"))
    return jax.shard_map(
        shards,
        mesh=mesh,
        in_specs=weights * 3 + (gain, gain),
        out_specs=(P("site", ("width", "zero")),) * 3
        + (P(("site", "width", "zero")),) * 3
        + (P("site"),),
        check_vma=False,
    )
```

```python
import functools

import jax
import jax.numpy as jnp
from jax import lax
from jax.experimental import pallas as pl
from jax.experimental.pallas import tpu as pltpu
from jax.sharding import PartitionSpec as P

D_MODEL = 7168
MIX_RATE = 1.0
ROWS = 224
COLS = 3584
OWN = 112
RANK = 64
PEERS = 32
HALF = PEERS // 2
BASE = (80, 88, 88)
BLOCK = OWN + max(BASE)
OVER = 3 * (OWN - BASE[0]) - BASE[0]
MESH = pl.DeviceIdType.MESH
VMEM_LIMIT = 56 << 20


def unit_of_lane(rows):
    return lax.broadcasted_iota(jnp.int32, (rows, 128), 1) // 32


def packed(block, free, base, more=()):
    first, tail = block[:, :128], block[:, 128:]
    spill = tail[base:]
    moved = jnp.concatenate(
        [pltpu.roll(spill, 128 - 32 * i, axis=1) for i in (1, 2, 3)] + list(more), axis=0
    )
    holds = min(base, moved.shape[0])
    mixed = jnp.where(unit_of_lane(holds) == free, moved[:holds], tail[:holds])
    rows = [first, mixed] + ([tail[holds:base]] if holds < base else [])
    rest = moved[holds:] if holds < moved.shape[0] else None
    return jnp.concatenate(rows, axis=0), rest


def unpacked(block, free, base, more=()):
    first, tail = block[:OWN], block[OWN : OWN + base]
    moved = jnp.concatenate([tail, *more], axis=0)
    size = OWN - base
    unit = unit_of_lane(size)
    spill = jnp.zeros((size, 128), jnp.float32)
    for i in (1, 2, 3):
        piece = pltpu.roll(moved[size * (i - 1) : size * i], 32 * i, axis=1)
        spill = jnp.where(unit == (free + i) % 4, piece, spill)
    return first, jnp.concatenate([tail, spill], axis=0)


def gather_columns(received, m, group, total, joined):
    lane = lax.broadcasted_iota(jnp.int32, (OWN, 128), 1)
    at = pl.multiple_of(group * 896, 128)
    parts = []
    for b in range(4):
        peer = group * 4 + b
        more = ()
        if m == 0:
            more = (received[1, peer, BLOCK - OVER :].astype(jnp.float32),)
        block = received[m, peer].astype(jnp.float32)
        parts.append(unpacked(block, 3 - b, BASE[m], more))
    tiles = []
    for b in range(4):
        tiles.append(parts[b][0])
        if b < 3:
            tiles.append(jnp.where(lane < 96 - 32 * b, parts[b][1], parts[b + 1][1]))
    for t, tile in enumerate(tiles):
        joined[:, pl.ds(at + 128 * t, 128)] = tile.astype(jnp.bfloat16)
        total = total + jnp.abs(tile)
    return total


def scale_of(sums):
    return jnp.sum(sums[...], axis=1, keepdims=True) / D_MODEL


def rescaled(joined, factor, final, i):
    window = pl.ds(pl.multiple_of(i * 896, 128), 896)
    final[:, window] = (joined[:, window].astype(jnp.float32) * factor).astype(jnp.bfloat16)


def as_row(scale):
    row = lax.broadcasted_iota(jnp.int32, (OWN, OWN), 0)
    column = lax.broadcasted_iota(jnp.int32, (OWN, OWN), 1)
    spread = jnp.broadcast_to(scale, (OWN, OWN))
    return jnp.sum(jnp.where(row == column, spread, 0.0), axis=0, keepdims=True)


def exchange(
    train_q, low_q, high_q, train_k, low_k, high_k, train_v, low_v, high_v, norm, step,
    joined_q, joined_k, joined_v, sums_v, scale_q, scale_k, serve,
    train, low, high, result, outgoing, received, sums, gains, over, rows,
    load_sem, low_sem, send_sem, recv_sem, gain_send, gain_recv, pair_send, pair_recv,
    across_send, across_recv,
):
    me = lax.axis_index("zero")
    width = lax.axis_index("width")
    site = lax.axis_index("site")
    far, y, x = me // 16, (me // 4) % 4, me % 4
    plane = me % 16
    sources = ((train_q, low_q, high_q), (train_k, low_k, high_k), (train_v, low_v, high_v))

    def group_of(s):
        return ((far + 1 + s // 2) % 2) * 2 + (y // 2 + s) % 2

    def loads(m, s):
        window = pl.ds(pl.multiple_of(group_of(s) * 896, 128), 896)
        return [
            pltpu.make_async_copy(
                sources[m][part].at[:, window], held.at[m, :, window], load_sem.at[m, s, i]
            )
            for i, (part, held) in enumerate(((0, train), (2, high)))
        ]

    def low_load(m):
        return pltpu.make_async_copy(sources[m][1], low.at[m], low_sem.at[m])

    def start_loads(m, s):
        if s == 0:
            low_load(m).start()
        for load in loads(m, s):
            load.start()

    start_loads(0, 0)
    barrier = pltpu.get_barrier_semaphore()

    def greet(i, carry):
        peer = (me + i) % PEERS
        pl.semaphore_signal(barrier, inc=1, device_id=(peer, width, site), device_id_type=MESH)
        return carry

    lax.fori_loop(1, PEERS, greet, 0)
    partner = (me, 1 - width, site)
    pl.semaphore_signal(barrier, inc=1, device_id=partner, device_id_type=MESH)
    for m in range(3):
        for s in range(4):
            if m or s:
                start_loads(m, s)

    from_row = lax.broadcasted_iota(jnp.int32, (ROWS, 256), 0)
    to_lane = lax.broadcasted_iota(jnp.int32, (ROWS, 256), 1)
    place = jnp.where(from_row == (to_lane + 32 * x) % 256, 1.0, 0.0).astype(jnp.bfloat16)

    gain = (norm[...] + step[...]).astype(jnp.bfloat16).astype(jnp.float32)
    gains[plane, far, pl.ds(width, 1), :] = jnp.concatenate(
        [gain, jnp.zeros((1, 128 - OWN), jnp.float32)], axis=1
    )

    def merge(m, group, turned_low):
        window = pl.ds(pl.multiple_of(group * 896, 128), 896)
        dims = (((0,), (0,)), ((), ()))
        result[...] = lax.dot_general(
            train[m, :, window], place, dims, preferred_element_type=jnp.float32
        ) + MIX_RATE * lax.dot_general(
            high[m, :, window], turned_low, dims, preferred_element_type=jnp.float32
        )

    def peer_of(group, j):
        return group * 8 + ((y + j // 4) % 2) * 4 + (x + j) % 4

    def pack(m, group, j):
        peer = peer_of(group, j)
        at = pl.multiple_of((peer - group * 8) * OWN, 8)
        more = (over[peer],) if m == 1 else ()
        rows_out, rest = packed(result[pl.ds(at, OWN), :], 3 - x, BASE[m], more)
        outgoing[m, peer, : OWN + BASE[m]] = rows_out.astype(jnp.bfloat16)
        if m == 0:
            over[peer] = rest

    def send(m, group, j, sem):
        peer = peer_of(group, j)

        @pl.when(peer != me)
        def _():
            pltpu.make_async_remote_copy(
                src_ref=outgoing.at[m, peer, pl.ds(0, OWN + BASE[m])],
                dst_ref=received.at[m, me, pl.ds(0, OWN + BASE[m])],
                send_sem=send_sem.at[m],
                recv_sem=recv_sem.at[m, sem],
                device_id=(peer, width, site),
                device_id_type=MESH,
            ).start()

    def across(end):
        return pltpu.make_async_remote_copy(
            src_ref=gains.at[plane, end],
            dst_ref=gains.at[plane, end],
            send_sem=across_send,
            recv_sem=across_recv,
            device_id=((me + HALF) % PEERS, width, site),
            device_id_type=MESH,
        )

    def spread(i, carry):
        pltpu.make_async_remote_copy(
            src_ref=gains.at[plane],
            dst_ref=gains.at[plane],
            send_sem=gain_send,
            recv_sem=gain_recv,
            device_id=(far * HALF + (plane + i) % HALF, width, site),
            device_id_type=MESH,
        ).start()
        return carry

    for m in range(3):
        for s in range(4):
            if s == 0:
                low_load(m).wait()
                turned_low = jnp.dot(
                    low[m], place, preferred_element_type=jnp.float32
                ).astype(jnp.bfloat16)
            for load in loads(m, s):
                load.wait()
            group = group_of(s)
            sem = y if s < 2 else 4
            merge(m, group, turned_low)
            pack(m, group, 0)
            if m == 0 and s == 0:
                pl.semaphore_wait(barrier, PEERS)

            def pack_and_send(j, carry, m=m, group=group, sem=sem):
                pack(m, group, j)
                send(m, group, j - 1, sem)
                return carry

            lax.fori_loop(1, 8, pack_and_send, 0)
            send(m, group, 7, sem)
            if m == 0 and s == 0:
                pltpu.make_async_remote_copy(
                    src_ref=gains.at[plane, far, pl.ds(width, 1)],
                    dst_ref=gains.at[plane, far, pl.ds(width, 1)],
                    send_sem=pair_send,
                    recv_sem=pair_recv,
                    device_id=partner,
                    device_id_type=MESH,
                ).start()
        if m == 0:
            pair = pltpu.make_async_remote_copy(
                src_ref=gains.at[plane, far, pl.ds(width, 1)],
                dst_ref=gains.at[plane, far, pl.ds(1 - width, 1)],
                send_sem=pair_send,
                recv_sem=pair_recv,
                device_id=partner,
                device_id_type=MESH,
            )
            pair.wait_recv()

            across(far).start()
        received[m, me] = outgoing[m, me]

    across(1 - far).wait_recv()
    lax.fori_loop(1, HALF, spread, 0)

    def arrived(m, sem, blocks):
        window = received.at[m, pl.ds(0, blocks), pl.ds(0, OWN + BASE[m])]
        pltpu.make_async_copy(window, window, recv_sem.at[m, sem]).wait()

    def gather_near(m, joined):
        if m == 2:
            arrived(m, 4, HALF - 1)
        sums[...] = lax.fori_loop(
            0,
            4,
            lambda i, total: gather_columns(received, m, far * 4 + i, total, joined),
            jnp.zeros((OWN, 128), jnp.float32),
        )

    def gather_far(m, joined):
        def one(i, carry):
            row = (y // 2 * 2 + (y + i) % 2 + i // 2 * 2) % 4
            if m == 2:
                arrived(m, row, 4)
            sums[...] = gather_columns(received, m, (1 - far) * 4 + row, sums[...], joined)
            return carry

        lax.fori_loop(0, 4, one, 0)

    for m in range(2):
        for sem in range(4):
            arrived(m, sem, 4)
        arrived(m, 4, HALF - 1)
    for m, (joined, scale_row) in enumerate(((joined_q, scale_q), (joined_k, scale_k))):
        gather_near(m, joined)
        gather_far(m, joined)
        scale = scale_of(sums)
        scale_row[...] = as_row(scale)
        factor = jnp.broadcast_to(1.0 / scale, (OWN, 896))

        def rescale(i, carry, joined=joined, factor=factor):
            rescaled(joined, factor, joined, i)
            return carry

        lax.fori_loop(0, 8, rescale, 0)

    gather_near(2, joined_v)
    spread_out = gains.at[pl.ds(0, HALF - 1)]
    pltpu.make_async_copy(spread_out, spread_out, gain_recv).wait()
    pltpu.make_async_copy(spread_out, spread_out, gain_send).wait()
    pair.wait_send()
    across(far).wait_send()
    lane = lax.broadcasted_iota(jnp.int32, (1, 128), 1)
    for r in range(D_MODEL // 128):
        place_in = r % 7
        first = r // 7 * 8 + place_in
        left, right = (
            gains[i // 2 % HALF, i // 2 // HALF, pl.ds(i % 2, 1), :] for i in (first, first + 1)
        )
        if place_in:
            left = pltpu.roll(left, 128 - 16 * place_in, axis=1)
        right = pltpu.roll(right, OWN - 16 * place_in, axis=1)
        rows[pl.ds(r, 1), :] = jnp.where(lane < OWN - 16 * place_in, left, right)
    serve[...] = rows[...].astype(jnp.bfloat16)

    for m in range(2):
        window = outgoing.at[m, pl.ds(0, PEERS - 1), pl.ds(0, OWN + BASE[m])]
        pltpu.make_async_copy(window, window, send_sem.at[m]).wait()
    gather_far(2, joined_v)
    sums_v[...] = sums[...]
    window = outgoing.at[2, pl.ds(0, PEERS - 1), pl.ds(0, OWN + BASE[2])]
    pltpu.make_async_copy(window, window, send_sem.at[2]).wait()


def finish(
    joined_q, joined_k, joined_v, sums_v, row_q, row_k, gain,
    final_q, final_k, final_v, scale_q, scale_k, scale_v, serve,
    last, row_v, sem,
):
    copies = [
        pltpu.make_async_copy(source, target, sem.at[i])
        for i, (source, target) in enumerate(
            (
                (row_q, scale_q), (row_k, scale_k), (gain, serve),
                (joined_q, final_q), (joined_k, final_k),
            )
        )
    ]
    for copy in copies:
        copy.start()
    scale = scale_of(sums_v)
    factor = jnp.broadcast_to(1.0 / scale, (OWN, 896))
    row_v[...] = as_row(scale)
    for i in range(8):
        rescaled(joined_v, factor, last, i)
        window = pl.ds(896 * i, 896)
        copies.append(
            pltpu.make_async_copy(last.at[:, window], final_v.at[:, window], sem.at[5 + i])
        )
        copies[-1].start()
        if i == 0:
            copies.append(pltpu.make_async_copy(row_v, scale_v, sem.at[13]))
            copies[-1].start()
    for copy in copies:
        copy.wait()


def shards(
    train_query, low_query, high_query,
    train_key, low_key, high_key,
    train_value, low_value, high_value,
    norm_train, norm_step,
):
    anywhere = pl.BlockSpec(memory_space=pl.ANY)
    vmem = pl.BlockSpec(memory_space=pltpu.VMEM)
    whole, row = (OWN, D_MODEL), (1, OWN)
    gain = (D_MODEL // 128, 128)
    dma = pltpu.SemaphoreType.DMA
    middle = pl.pallas_call(
        exchange,
        name="exchange",
        out_shape=(
            *[pltpu.VMEM(whole, jnp.bfloat16)] * 3,
            pltpu.VMEM((OWN, 128), jnp.float32),
            *[pltpu.VMEM(row, jnp.float32)] * 2,
            pltpu.VMEM(gain, jnp.bfloat16),
        ),
        in_specs=[anywhere] * 9 + [vmem] * 2,
        out_specs=(vmem,) * 7,
        scratch_shapes=[
            pltpu.VMEM((3, ROWS, COLS), jnp.bfloat16),
            pltpu.VMEM((3, RANK, ROWS), jnp.bfloat16),
            pltpu.VMEM((3, RANK, COLS), jnp.bfloat16),
            pltpu.VMEM((896, 256), jnp.float32),
            pltpu.VMEM((3, PEERS, BLOCK, 128), jnp.bfloat16),
            pltpu.VMEM((3, PEERS, BLOCK, 128), jnp.bfloat16),
            pltpu.VMEM((OWN, 128), jnp.float32),
            pltpu.VMEM((HALF, 2, 2, 128), jnp.float32),
            pltpu.VMEM((PEERS, OVER, 128), jnp.float32),
            pltpu.VMEM(gain, jnp.float32),
            dma((3, 4, 2)), dma((3,)), dma((3,)), dma((3, 5)), *[dma] * 6,
        ],
        compiler_params=pltpu.CompilerParams(
            collective_id=0, has_side_effects=True, vmem_limit_bytes=VMEM_LIMIT
        ),
    )(
        train_query, low_query.T, high_query,
        train_key, low_key.T, high_key,
        train_value, low_value.T, high_value,
        norm_train.reshape(row), norm_step.reshape(row),
    )
    *finals, scale_q, scale_k, scale_v, serve = pl.pallas_call(
        finish,
        name="finish",
        out_shape=(
            *[jax.ShapeDtypeStruct(whole, jnp.bfloat16)] * 3,
            *[jax.ShapeDtypeStruct(row, jnp.float32)] * 3,
            jax.ShapeDtypeStruct(gain, jnp.bfloat16),
        ),
        in_specs=[vmem] * 7,
        out_specs=(anywhere,) * 7,
        scratch_shapes=[
            pltpu.VMEM(whole, jnp.bfloat16), pltpu.VMEM(row, jnp.float32), dma((14,)),
        ],
        compiler_params=pltpu.CompilerParams(vmem_limit_bytes=16 << 20),
    )(*middle)
    return (
        *[final.T for final in finals],
        scale_q.reshape(OWN), scale_k.reshape(OWN), scale_v.reshape(OWN),
        serve.reshape(D_MODEL),
    )


def solution(mesh):
    weights = (P(("site", "zero"), "width"), P(("site", "zero"), None), P("site", "width"))
    gain = P(("site", "zero", "width"))
    return jax.shard_map(
        shards,
        mesh=mesh,
        in_specs=weights * 3 + (gain, gain),
        out_specs=(P("site", ("width", "zero")),) * 3
        + (P(("site", "width", "zero")),) * 3
        + (P("site"),),
        check_vma=False,
    )
```

```python
import functools

import jax
import jax.numpy as jnp
from jax import lax
from jax.experimental import pallas as pl
from jax.experimental.pallas import tpu as pltpu
from jax.sharding import PartitionSpec as P

D_MODEL = 7168
MIX_RATE = 1.0
ROWS = 224
COLS = 3584
OWN = 112
RANK = 64
PEERS = 32
HALF = PEERS // 2
BASE = (80, 88, 88)
BLOCK = OWN + max(BASE)
OVER = 3 * (OWN - BASE[0]) - BASE[0]
FAR_FIRST = sorted(
    ((dy, dx) for dy in range(4) for dx in range(4)),
    key=lambda hop: -(min(hop[0], 4 - hop[0]) + min(hop[1], 4 - hop[1])),
)
MESH = pl.DeviceIdType.MESH
VMEM_LIMIT = 56 << 20


def unit_of_lane(rows):
    return lax.broadcasted_iota(jnp.int32, (rows, 128), 1) // 32


def packed(block, free, base, more=()):
    first, tail = block[:, :128], block[:, 128:]
    spill = tail[base:]
    moved = jnp.concatenate(
        [pltpu.roll(spill, 128 - 32 * i, axis=1) for i in (1, 2, 3)] + list(more), axis=0
    )
    holds = min(base, moved.shape[0])
    mixed = jnp.where(unit_of_lane(holds) == free, moved[:holds], tail[:holds])
    rows = [first, mixed] + ([tail[holds:base]] if holds < base else [])
    rest = moved[holds:] if holds < moved.shape[0] else None
    return jnp.concatenate(rows, axis=0), rest


def unpacked(block, free, base, more=()):
    first, tail = block[:OWN], block[OWN : OWN + base]
    moved = jnp.concatenate([tail, *more], axis=0)
    size = OWN - base
    unit = unit_of_lane(size)
    spill = jnp.zeros((size, 128), jnp.float32)
    for i in (1, 2, 3):
        piece = pltpu.roll(moved[size * (i - 1) : size * i], 32 * i, axis=1)
        spill = jnp.where(unit == (free + i) % 4, piece, spill)
    return first, jnp.concatenate([tail, spill], axis=0)


def gather_columns(received, m, group, total, joined):
    lane = lax.broadcasted_iota(jnp.int32, (OWN, 128), 1)
    at = pl.multiple_of(group * 896, 128)
    parts = []
    for b in range(4):
        peer = group * 4 + b
        more = ()
        if m == 0:
            more = (received[1, peer, BLOCK - OVER :].astype(jnp.float32),)
        block = received[m, peer].astype(jnp.float32)
        parts.append(unpacked(block, 3 - b, BASE[m], more))
    tiles = []
    for b in range(4):
        tiles.append(parts[b][0])
        if b < 3:
            tiles.append(jnp.where(lane < 96 - 32 * b, parts[b][1], parts[b + 1][1]))
    for t, tile in enumerate(tiles):
        joined[:, pl.ds(at + 128 * t, 128)] = tile.astype(jnp.bfloat16)
        total = total + jnp.abs(tile)
    return total


def scale_of(sums):
    return jnp.sum(sums[...], axis=1, keepdims=True) / D_MODEL


def rescaled(joined, factor, final, i):
    window = pl.ds(pl.multiple_of(i * 896, 128), 896)
    final[:, window] = (joined[:, window].astype(jnp.float32) * factor).astype(jnp.bfloat16)


def as_row(scale):
    row = lax.broadcasted_iota(jnp.int32, (OWN, OWN), 0)
    column = lax.broadcasted_iota(jnp.int32, (OWN, OWN), 1)
    spread = jnp.broadcast_to(scale, (OWN, OWN))
    return jnp.sum(jnp.where(row == column, spread, 0.0), axis=0, keepdims=True)


def exchange(
    train_q, low_q, high_q, train_k, low_k, high_k, train_v, low_v, high_v, norm, step,
    joined_q, joined_k, joined_v, sums_v, scale_q, scale_k, serve,
    train, low, high, result, outgoing, received, sums, gains, over, rows,
    load_sem, low_sem, send_sem, recv_sem, gain_send, gain_recv, pair_send, pair_recv,
    across_send, across_recv,
):
    me = lax.axis_index("zero")
    width = lax.axis_index("width")
    site = lax.axis_index("site")
    far, y, x = me // 16, (me // 4) % 4, me % 4
    plane = me % 16
    sources = ((train_q, low_q, high_q), (train_k, low_k, high_k), (train_v, low_v, high_v))

    def group_of(s):
        return ((far + 1 + s // 2) % 2) * 2 + (y // 2 + s) % 2

    def loads(m, s):
        window = pl.ds(pl.multiple_of(group_of(s) * 896, 128), 896)
        return [
            pltpu.make_async_copy(
                sources[m][part].at[:, window], held.at[m, :, window], load_sem.at[m, s, i]
            )
            for i, (part, held) in enumerate(((0, train), (2, high)))
        ]

    def low_load(m):
        return pltpu.make_async_copy(sources[m][1], low.at[m], low_sem.at[m])

    def start_loads(m, s):
        if s == 0:
            low_load(m).start()
        for load in loads(m, s):
            load.start()

    start_loads(0, 0)
    barrier = pltpu.get_barrier_semaphore()

    def greet(i, carry):
        peer = (me + i) % PEERS
        pl.semaphore_signal(barrier, inc=1, device_id=(peer, width, site), device_id_type=MESH)
        return carry

    lax.fori_loop(1, PEERS, greet, 0)
    partner = (me, 1 - width, site)
    pl.semaphore_signal(barrier, inc=1, device_id=partner, device_id_type=MESH)
    for m in range(3):
        for s in range(4):
            if m or s:
                start_loads(m, s)

    from_row = lax.broadcasted_iota(jnp.int32, (ROWS, 256), 0)
    to_lane = lax.broadcasted_iota(jnp.int32, (ROWS, 256), 1)
    place = jnp.where(from_row == (to_lane + 32 * x) % 256, 1.0, 0.0).astype(jnp.bfloat16)

    gain = (norm[...] + step[...]).astype(jnp.bfloat16).astype(jnp.float32)
    gains[plane, far, pl.ds(width, 1), :] = jnp.concatenate(
        [gain, jnp.zeros((1, 128 - OWN), jnp.float32)], axis=1
    )

    def merge(m, group, turned_low):
        window = pl.ds(pl.multiple_of(group * 896, 128), 896)
        dims = (((0,), (0,)), ((), ()))
        result[...] = lax.dot_general(
            train[m, :, window], place, dims, preferred_element_type=jnp.float32
        ) + MIX_RATE * lax.dot_general(
            high[m, :, window], turned_low, dims, preferred_element_type=jnp.float32
        )

    def pack(m, group, j):
        peer = group * 8 + j
        at = pl.multiple_of(j * OWN, 8)
        more = (over[peer],) if m == 1 else ()
        rows_out, rest = packed(result[pl.ds(at, OWN), :], 3 - x, BASE[m], more)
        outgoing[m, peer, : OWN + BASE[m]] = rows_out.astype(jnp.bfloat16)
        if m == 0:
            over[peer] = rest

    def send(m, plane_z, dy, dx, sem):
        peer = plane_z * HALF + (y + dy) % 4 * 4 + (x + dx) % 4
        pltpu.make_async_remote_copy(
            src_ref=outgoing.at[m, peer, pl.ds(0, OWN + BASE[m])],
            dst_ref=received.at[m, me, pl.ds(0, OWN + BASE[m])],
            send_sem=send_sem.at[m],
            recv_sem=recv_sem.at[m, sem],
            device_id=(peer, width, site),
            device_id_type=MESH,
        ).start()

    def across(end):
        return pltpu.make_async_remote_copy(
            src_ref=gains.at[plane, end],
            dst_ref=gains.at[plane, end],
            send_sem=across_send,
            recv_sem=across_recv,
            device_id=((me + HALF) % PEERS, width, site),
            device_id_type=MESH,
        )

    def spread(i, carry):
        pltpu.make_async_remote_copy(
            src_ref=gains.at[plane],
            dst_ref=gains.at[plane],
            send_sem=gain_send,
            recv_sem=gain_recv,
            device_id=(far * HALF + (plane + i) % HALF, width, site),
            device_id_type=MESH,
        ).start()
        return carry

    for m in range(3):
        for s in range(4):
            if s == 0:
                low_load(m).wait()
                turned_low = jnp.dot(
                    low[m], place, preferred_element_type=jnp.float32
                ).astype(jnp.bfloat16)
            for load in loads(m, s):
                load.wait()
            group = group_of(s)
            merge(m, group, turned_low)

            def pack_one(j, carry, m=m, group=group):
                pack(m, group, j)
                return carry

            lax.fori_loop(0, 8, pack_one, 0)
            if s % 2 == 0:
                continue
            if m == 0 and s == 1:
                pl.semaphore_wait(barrier, PEERS)
            for dy, dx in FAR_FIRST:
                if s == 1:
                    send(m, 1 - far, dy, dx, y)
                elif dy or dx:
                    send(m, far, dy, dx, 4)
            if m == 0 and s == 1:
                pltpu.make_async_remote_copy(
                    src_ref=gains.at[plane, far, pl.ds(width, 1)],
                    dst_ref=gains.at[plane, far, pl.ds(width, 1)],
                    send_sem=pair_send,
                    recv_sem=pair_recv,
                    device_id=partner,
                    device_id_type=MESH,
                ).start()
        if m == 0:
            pair = pltpu.make_async_remote_copy(
                src_ref=gains.at[plane, far, pl.ds(width, 1)],
                dst_ref=gains.at[plane, far, pl.ds(1 - width, 1)],
                send_sem=pair_send,
                recv_sem=pair_recv,
                device_id=partner,
                device_id_type=MESH,
            )
            pair.wait_recv()

            across(far).start()
        received[m, me] = outgoing[m, me]

    across(1 - far).wait_recv()
    lax.fori_loop(1, HALF, spread, 0)

    def arrived(m, sem, blocks):
        window = received.at[m, pl.ds(0, blocks), pl.ds(0, OWN + BASE[m])]
        pltpu.make_async_copy(window, window, recv_sem.at[m, sem]).wait()

    def gather_near(m, joined):
        if m == 2:
            arrived(m, 4, HALF - 1)
        sums[...] = lax.fori_loop(
            0,
            4,
            lambda i, total: gather_columns(received, m, far * 4 + i, total, joined),
            jnp.zeros((OWN, 128), jnp.float32),
        )

    def gather_far(m, joined):
        def one(i, carry):
            row = (y + 2 - i % 2 + i // 2 * 2) % 4
            if m == 2:
                arrived(m, row, 4)
            sums[...] = gather_columns(received, m, (1 - far) * 4 + row, sums[...], joined)
            return carry

        lax.fori_loop(0, 4, one, 0)

    for m in range(2):
        for sem in range(4):
            arrived(m, sem, 4)
        arrived(m, 4, HALF - 1)
    for m, (joined, scale_row) in enumerate(((joined_q, scale_q), (joined_k, scale_k))):
        gather_near(m, joined)
        gather_far(m, joined)
        scale = scale_of(sums)
        scale_row[...] = as_row(scale)
        factor = jnp.broadcast_to(1.0 / scale, (OWN, 896))

        def rescale(i, carry, joined=joined, factor=factor):
            rescaled(joined, factor, joined, i)
            return carry

        lax.fori_loop(0, 8, rescale, 0)

    gather_near(2, joined_v)
    spread_out = gains.at[pl.ds(0, HALF - 1)]
    pltpu.make_async_copy(spread_out, spread_out, gain_recv).wait()
    pltpu.make_async_copy(spread_out, spread_out, gain_send).wait()
    pair.wait_send()
    across(far).wait_send()
    lane = lax.broadcasted_iota(jnp.int32, (1, 128), 1)
    for r in range(D_MODEL // 128):
        place_in = r % 7
        first = r // 7 * 8 + place_in
        left, right = (
            gains[i // 2 % HALF, i // 2 // HALF, pl.ds(i % 2, 1), :] for i in (first, first + 1)
        )
        if place_in:
            left = pltpu.roll(left, 128 - 16 * place_in, axis=1)
        right = pltpu.roll(right, OWN - 16 * place_in, axis=1)
        rows[pl.ds(r, 1), :] = jnp.where(lane < OWN - 16 * place_in, left, right)
    serve[...] = rows[...].astype(jnp.bfloat16)

    for m in range(2):
        window = outgoing.at[m, pl.ds(0, PEERS - 1), pl.ds(0, OWN + BASE[m])]
        pltpu.make_async_copy(window, window, send_sem.at[m]).wait()
    gather_far(2, joined_v)
    sums_v[...] = sums[...]
    window = outgoing.at[2, pl.ds(0, PEERS - 1), pl.ds(0, OWN + BASE[2])]
    pltpu.make_async_copy(window, window, send_sem.at[2]).wait()


def finish(
    joined_q, joined_k, joined_v, sums_v, row_q, row_k, gain,
    final_q, final_k, final_v, scale_q, scale_k, scale_v, serve,
    last, row_v, sem,
):
    copies = [
        pltpu.make_async_copy(source, target, sem.at[i])
        for i, (source, target) in enumerate(
            (
                (row_q, scale_q), (row_k, scale_k), (gain, serve),
                (joined_q, final_q), (joined_k, final_k),
            )
        )
    ]
    for copy in copies:
        copy.start()
    scale = scale_of(sums_v)
    factor = jnp.broadcast_to(1.0 / scale, (OWN, 896))
    row_v[...] = as_row(scale)
    for i in range(8):
        rescaled(joined_v, factor, last, i)
        window = pl.ds(896 * i, 896)
        copies.append(
            pltpu.make_async_copy(last.at[:, window], final_v.at[:, window], sem.at[5 + i])
        )
        copies[-1].start()
        if i == 0:
            copies.append(pltpu.make_async_copy(row_v, scale_v, sem.at[13]))
            copies[-1].start()
    for copy in copies:
        copy.wait()


def shards(
    train_query, low_query, high_query,
    train_key, low_key, high_key,
    train_value, low_value, high_value,
    norm_train, norm_step,
):
    anywhere = pl.BlockSpec(memory_space=pl.ANY)
    vmem = pl.BlockSpec(memory_space=pltpu.VMEM)
    whole, row = (OWN, D_MODEL), (1, OWN)
    gain = (D_MODEL // 128, 128)
    dma = pltpu.SemaphoreType.DMA
    middle = pl.pallas_call(
        exchange,
        name="exchange",
        out_shape=(
            *[pltpu.VMEM(whole, jnp.bfloat16)] * 3,
            pltpu.VMEM((OWN, 128), jnp.float32),
            *[pltpu.VMEM(row, jnp.float32)] * 2,
            pltpu.VMEM(gain, jnp.bfloat16),
        ),
        in_specs=[anywhere] * 9 + [vmem] * 2,
        out_specs=(vmem,) * 7,
        scratch_shapes=[
            pltpu.VMEM((3, ROWS, COLS), jnp.bfloat16),
            pltpu.VMEM((3, RANK, ROWS), jnp.bfloat16),
            pltpu.VMEM((3, RANK, COLS), jnp.bfloat16),
            pltpu.VMEM((896, 256), jnp.float32),
            pltpu.VMEM((3, PEERS, BLOCK, 128), jnp.bfloat16),
            pltpu.VMEM((3, PEERS, BLOCK, 128), jnp.bfloat16),
            pltpu.VMEM((OWN, 128), jnp.float32),
            pltpu.VMEM((HALF, 2, 2, 128), jnp.float32),
            pltpu.VMEM((PEERS, OVER, 128), jnp.float32),
            pltpu.VMEM(gain, jnp.float32),
            dma((3, 4, 2)), dma((3,)), dma((3,)), dma((3, 5)), *[dma] * 6,
        ],
        compiler_params=pltpu.CompilerParams(
            collective_id=0, has_side_effects=True, vmem_limit_bytes=VMEM_LIMIT
        ),
    )(
        train_query, low_query.T, high_query,
        train_key, low_key.T, high_key,
        train_value, low_value.T, high_value,
        norm_train.reshape(row), norm_step.reshape(row),
    )
    *finals, scale_q, scale_k, scale_v, serve = pl.pallas_call(
        finish,
        name="finish",
        out_shape=(
            *[jax.ShapeDtypeStruct(whole, jnp.bfloat16)] * 3,
            *[jax.ShapeDtypeStruct(row, jnp.float32)] * 3,
            jax.ShapeDtypeStruct(gain, jnp.bfloat16),
        ),
        in_specs=[vmem] * 7,
        out_specs=(anywhere,) * 7,
        scratch_shapes=[
            pltpu.VMEM(whole, jnp.bfloat16), pltpu.VMEM(row, jnp.float32), dma((14,)),
        ],
        compiler_params=pltpu.CompilerParams(vmem_limit_bytes=16 << 20),
    )(*middle)
    return (
        *[final.T for final in finals],
        scale_q.reshape(OWN), scale_k.reshape(OWN), scale_v.reshape(OWN),
        serve.reshape(D_MODEL),
    )


def solution(mesh):
    weights = (P(("site", "zero"), "width"), P(("site", "zero"), None), P("site", "width"))
    gain = P(("site", "zero", "width"))
    return jax.shard_map(
        shards,
        mesh=mesh,
        in_specs=weights * 3 + (gain, gain),
        out_specs=(P("site", ("width", "zero")),) * 3
        + (P(("site", "width", "zero")),) * 3
        + (P("site"),),
        check_vma=False,
    )
```

```python
import functools

import jax
import jax.numpy as jnp
from jax import lax
from jax.experimental import pallas as pl
from jax.experimental.pallas import tpu as pltpu
from jax.sharding import PartitionSpec as P

D_MODEL = 7168
MIX_RATE = 1.0
ROWS = 224
COLS = 3584
OWN = 112
RANK = 64
PEERS = 32
HALF = PEERS // 2
BASE = (80, 88, 88)
BLOCK = OWN + max(BASE)
OVER = 3 * (OWN - BASE[0]) - BASE[0]
FAR_FIRST = sorted(
    ((dy, dx) for dy in range(4) for dx in range(4)),
    key=lambda hop: -(min(hop[0], 4 - hop[0]) + min(hop[1], 4 - hop[1])),
)
MESH = pl.DeviceIdType.MESH
VMEM_LIMIT = 56 << 20


def unit_of_lane(rows):
    return lax.broadcasted_iota(jnp.int32, (rows, 128), 1) // 32


def packed(block, free, base, more=()):
    first, tail = block[:, :128], block[:, 128:]
    spill = tail[base:]
    moved = jnp.concatenate(
        [pltpu.roll(spill, 128 - 32 * i, axis=1) for i in (1, 2, 3)] + list(more), axis=0
    )
    holds = min(base, moved.shape[0])
    mixed = jnp.where(unit_of_lane(holds) == free, moved[:holds], tail[:holds])
    rows = [first, mixed] + ([tail[holds:base]] if holds < base else [])
    rest = moved[holds:] if holds < moved.shape[0] else None
    return jnp.concatenate(rows, axis=0), rest


def unpacked(block, free, base, more=()):
    first, tail = block[:OWN], block[OWN : OWN + base]
    moved = jnp.concatenate([tail, *more], axis=0)
    size = OWN - base
    unit = unit_of_lane(size)
    spill = jnp.zeros((size, 128), jnp.float32)
    for i in (1, 2, 3):
        piece = pltpu.roll(moved[size * (i - 1) : size * i], 32 * i, axis=1)
        spill = jnp.where(unit == (free + i) % 4, piece, spill)
    return first, jnp.concatenate([tail, spill], axis=0)


def gather_columns(received, m, group, total, joined):
    lane = lax.broadcasted_iota(jnp.int32, (OWN, 128), 1)
    at = pl.multiple_of(group * 896, 128)
    parts = []
    for b in range(4):
        peer = group * 4 + b
        more = ()
        if m == 0:
            more = (received[1, peer, BLOCK - OVER :].astype(jnp.float32),)
        block = received[m, peer].astype(jnp.float32)
        parts.append(unpacked(block, 3 - b, BASE[m], more))
    tiles = []
    for b in range(4):
        tiles.append(parts[b][0])
        if b < 3:
            tiles.append(jnp.where(lane < 96 - 32 * b, parts[b][1], parts[b + 1][1]))
    for t, tile in enumerate(tiles):
        joined[:, pl.ds(at + 128 * t, 128)] = tile.astype(jnp.bfloat16)
        total = total + jnp.abs(tile)
    return total


def scale_of(sums):
    return jnp.sum(sums[...], axis=1, keepdims=True) / D_MODEL


def rescaled(joined, factor, final, i):
    window = pl.ds(pl.multiple_of(i * 896, 128), 896)
    final[:, window] = (joined[:, window].astype(jnp.float32) * factor).astype(jnp.bfloat16)


def as_row(scale):
    row = lax.broadcasted_iota(jnp.int32, (OWN, OWN), 0)
    column = lax.broadcasted_iota(jnp.int32, (OWN, OWN), 1)
    spread = jnp.broadcast_to(scale, (OWN, OWN))
    return jnp.sum(jnp.where(row == column, spread, 0.0), axis=0, keepdims=True)


def exchange(
    train_q, low_q, high_q, train_k, low_k, high_k, train_v, low_v, high_v, norm, step,
    joined_q, joined_k, joined_v, sums_v, scale_q, scale_k, serve,
    train, low, high, result, outgoing, received, sums, gains, over, rows,
    load_sem, low_sem, send_sem, recv_sem, gain_send, gain_recv, pair_send, pair_recv,
    across_send, across_recv,
):
    me = lax.axis_index("zero")
    width = lax.axis_index("width")
    site = lax.axis_index("site")
    far, y, x = me // 16, (me // 4) % 4, me % 4
    plane = me % 16
    sources = ((train_q, low_q, high_q), (train_k, low_k, high_k), (train_v, low_v, high_v))

    def group_of(s):
        return ((far + 1 + s // 2) % 2) * 2 + (y // 2 + s) % 2

    def loads(m, s):
        window = pl.ds(pl.multiple_of(group_of(s) * 896, 128), 896)
        return [
            pltpu.make_async_copy(
                sources[m][part].at[:, window], held.at[m, :, window], load_sem.at[m, s, i]
            )
            for i, (part, held) in enumerate(((0, train), (2, high)))
        ]

    def low_load(m):
        return pltpu.make_async_copy(sources[m][1], low.at[m], low_sem.at[m])

    def start_loads(m, s):
        if s == 0:
            low_load(m).start()
        for load in loads(m, s):
            load.start()

    start_loads(0, 0)
    barrier = pltpu.get_barrier_semaphore()

    def greet(i, carry):
        peer = (me + i) % PEERS
        pl.semaphore_signal(barrier, inc=1, device_id=(peer, width, site), device_id_type=MESH)
        return carry

    lax.fori_loop(1, PEERS, greet, 0)
    partner = (me, 1 - width, site)
    pl.semaphore_signal(barrier, inc=1, device_id=partner, device_id_type=MESH)
    for m in range(3):
        for s in range(4):
            if m or s:
                start_loads(m, s)

    from_row = lax.broadcasted_iota(jnp.int32, (ROWS, 256), 0)
    to_lane = lax.broadcasted_iota(jnp.int32, (ROWS, 256), 1)
    place = jnp.where(from_row == (to_lane + 32 * x) % 256, 1.0, 0.0).astype(jnp.bfloat16)

    gain = (norm[...] + step[...]).astype(jnp.bfloat16).astype(jnp.float32)
    gains[plane, far, pl.ds(width, 1), :] = jnp.concatenate(
        [gain, jnp.zeros((1, 128 - OWN), jnp.float32)], axis=1
    )

    def merge(m, group, turned_low):
        window = pl.ds(pl.multiple_of(group * 896, 128), 896)
        dims = (((0,), (0,)), ((), ()))
        result[...] = lax.dot_general(
            train[m, :, window], place, dims, preferred_element_type=jnp.float32
        ) + MIX_RATE * lax.dot_general(
            high[m, :, window], turned_low, dims, preferred_element_type=jnp.float32
        )

    def pack(m, group, j):
        peer = group * 8 + j
        at = pl.multiple_of(j * OWN, 8)
        more = (over[peer],) if m == 1 else ()
        rows_out, rest = packed(result[pl.ds(at, OWN), :], 3 - x, BASE[m], more)
        outgoing[m, peer, : OWN + BASE[m]] = rows_out.astype(jnp.bfloat16)
        if m == 0:
            over[peer] = rest

    def send(m, plane_z, dy, dx, sem):
        peer = plane_z * HALF + (y + dy) % 4 * 4 + (x + dx) % 4
        pltpu.make_async_remote_copy(
            src_ref=outgoing.at[m, peer, pl.ds(0, OWN + BASE[m])],
            dst_ref=received.at[m, me, pl.ds(0, OWN + BASE[m])],
            send_sem=send_sem.at[m],
            recv_sem=recv_sem.at[m, sem],
            device_id=(peer, width, site),
            device_id_type=MESH,
        ).start()

    def across(end):
        return pltpu.make_async_remote_copy(
            src_ref=gains.at[plane, end],
            dst_ref=gains.at[plane, end],
            send_sem=across_send,
            recv_sem=across_recv,
            device_id=((me + HALF) % PEERS, width, site),
            device_id_type=MESH,
        )

    def spread(i, carry):
        pltpu.make_async_remote_copy(
            src_ref=gains.at[plane],
            dst_ref=gains.at[plane],
            send_sem=gain_send,
            recv_sem=gain_recv,
            device_id=(far * HALF + (plane + i) % HALF, width, site),
            device_id_type=MESH,
        ).start()
        return carry

    for m in range(3):
        low_load(m).wait()
        turned_low = jnp.dot(low[m], place, preferred_element_type=jnp.float32).astype(
            jnp.bfloat16
        )

        def prepare(s, carry, m=m, turned_low=turned_low):
            for load in loads(m, s):
                load.wait()
            group = group_of(s)
            merge(m, group, turned_low)

            def pack_one(j, inner):
                pack(m, group, j)
                return inner

            return lax.fori_loop(0, 8, pack_one, carry)

        for half in range(2):
            lax.fori_loop(2 * half, 2 * half + 2, prepare, 0)
            if m == 0 and half == 0:
                pl.semaphore_wait(barrier, PEERS)
            for dy, dx in FAR_FIRST:
                if half == 0:
                    send(m, 1 - far, dy, dx, y)
                elif dy or dx:
                    send(m, far, dy, dx, 4)
            if m == 0 and half == 0:
                pltpu.make_async_remote_copy(
                    src_ref=gains.at[plane, far, pl.ds(width, 1)],
                    dst_ref=gains.at[plane, far, pl.ds(width, 1)],
                    send_sem=pair_send,
                    recv_sem=pair_recv,
                    device_id=partner,
                    device_id_type=MESH,
                ).start()
        if m == 0:
            pair = pltpu.make_async_remote_copy(
                src_ref=gains.at[plane, far, pl.ds(width, 1)],
                dst_ref=gains.at[plane, far, pl.ds(1 - width, 1)],
                send_sem=pair_send,
                recv_sem=pair_recv,
                device_id=partner,
                device_id_type=MESH,
            )
            pair.wait_recv()

            across(far).start()
        received[m, me] = outgoing[m, me]

    across(1 - far).wait_recv()
    lax.fori_loop(1, HALF, spread, 0)

    def arrived(m, sem, blocks):
        window = received.at[m, pl.ds(0, blocks), pl.ds(0, OWN + BASE[m])]
        pltpu.make_async_copy(window, window, recv_sem.at[m, sem]).wait()

    def gather_near(m, joined):
        if m == 2:
            arrived(m, 4, HALF - 1)
        sums[...] = lax.fori_loop(
            0,
            4,
            lambda i, total: gather_columns(received, m, far * 4 + i, total, joined),
            jnp.zeros((OWN, 128), jnp.float32),
        )

    def gather_far(m, joined):
        def one(i, carry):
            row = (y + 2 - i % 2 + i // 2 * 2) % 4
            if m == 2:
                arrived(m, row, 4)
            sums[...] = gather_columns(received, m, (1 - far) * 4 + row, sums[...], joined)
            return carry

        lax.fori_loop(0, 4, one, 0)

    for m in range(2):
        for sem in range(4):
            arrived(m, sem, 4)
        arrived(m, 4, HALF - 1)
    for m, (joined, scale_row) in enumerate(((joined_q, scale_q), (joined_k, scale_k))):
        gather_near(m, joined)
        gather_far(m, joined)
        scale = scale_of(sums)
        scale_row[...] = as_row(scale)
        factor = jnp.broadcast_to(1.0 / scale, (OWN, 896))

        def rescale(i, carry, joined=joined, factor=factor):
            rescaled(joined, factor, joined, i)
            return carry

        lax.fori_loop(0, 8, rescale, 0)

    gather_near(2, joined_v)
    spread_out = gains.at[pl.ds(0, HALF - 1)]
    pltpu.make_async_copy(spread_out, spread_out, gain_recv).wait()
    pltpu.make_async_copy(spread_out, spread_out, gain_send).wait()
    pair.wait_send()
    across(far).wait_send()
    lane = lax.broadcasted_iota(jnp.int32, (1, 128), 1)
    for r in range(D_MODEL // 128):
        place_in = r % 7
        first = r // 7 * 8 + place_in
        left, right = (
            gains[i // 2 % HALF, i // 2 // HALF, pl.ds(i % 2, 1), :] for i in (first, first + 1)
        )
        if place_in:
            left = pltpu.roll(left, 128 - 16 * place_in, axis=1)
        right = pltpu.roll(right, OWN - 16 * place_in, axis=1)
        rows[pl.ds(r, 1), :] = jnp.where(lane < OWN - 16 * place_in, left, right)
    serve[...] = rows[...].astype(jnp.bfloat16)

    for m in range(2):
        window = outgoing.at[m, pl.ds(0, PEERS - 1), pl.ds(0, OWN + BASE[m])]
        pltpu.make_async_copy(window, window, send_sem.at[m]).wait()
    gather_far(2, joined_v)
    sums_v[...] = sums[...]
    window = outgoing.at[2, pl.ds(0, PEERS - 1), pl.ds(0, OWN + BASE[2])]
    pltpu.make_async_copy(window, window, send_sem.at[2]).wait()


def finish(
    joined_q, joined_k, joined_v, sums_v, row_q, row_k, gain,
    final_q, final_k, final_v, scale_q, scale_k, scale_v, serve,
    last, row_v, sem,
):
    copies = [
        pltpu.make_async_copy(source, target, sem.at[i])
        for i, (source, target) in enumerate(
            (
                (row_q, scale_q), (row_k, scale_k), (gain, serve),
                (joined_q, final_q), (joined_k, final_k),
            )
        )
    ]
    for copy in copies:
        copy.start()
    scale = scale_of(sums_v)
    factor = jnp.broadcast_to(1.0 / scale, (OWN, 896))
    row_v[...] = as_row(scale)
    for i in range(8):
        rescaled(joined_v, factor, last, i)
        window = pl.ds(896 * i, 896)
        copies.append(
            pltpu.make_async_copy(last.at[:, window], final_v.at[:, window], sem.at[5 + i])
        )
        copies[-1].start()
        if i == 0:
            copies.append(pltpu.make_async_copy(row_v, scale_v, sem.at[13]))
            copies[-1].start()
    for copy in copies:
        copy.wait()


def shards(
    train_query, low_query, high_query,
    train_key, low_key, high_key,
    train_value, low_value, high_value,
    norm_train, norm_step,
):
    anywhere = pl.BlockSpec(memory_space=pl.ANY)
    vmem = pl.BlockSpec(memory_space=pltpu.VMEM)
    whole, row = (OWN, D_MODEL), (1, OWN)
    gain = (D_MODEL // 128, 128)
    dma = pltpu.SemaphoreType.DMA
    middle = pl.pallas_call(
        exchange,
        name="exchange",
        out_shape=(
            *[pltpu.VMEM(whole, jnp.bfloat16)] * 3,
            pltpu.VMEM((OWN, 128), jnp.float32),
            *[pltpu.VMEM(row, jnp.float32)] * 2,
            pltpu.VMEM(gain, jnp.bfloat16),
        ),
        in_specs=[anywhere] * 9 + [vmem] * 2,
        out_specs=(vmem,) * 7,
        scratch_shapes=[
            pltpu.VMEM((3, ROWS, COLS), jnp.bfloat16),
            pltpu.VMEM((3, RANK, ROWS), jnp.bfloat16),
            pltpu.VMEM((3, RANK, COLS), jnp.bfloat16),
            pltpu.VMEM((896, 256), jnp.float32),
            pltpu.VMEM((3, PEERS, BLOCK, 128), jnp.bfloat16),
            pltpu.VMEM((3, PEERS, BLOCK, 128), jnp.bfloat16),
            pltpu.VMEM((OWN, 128), jnp.float32),
            pltpu.VMEM((HALF, 2, 2, 128), jnp.float32),
            pltpu.VMEM((PEERS, OVER, 128), jnp.float32),
            pltpu.VMEM(gain, jnp.float32),
            dma((3, 4, 2)), dma((3,)), dma((3,)), dma((3, 5)), *[dma] * 6,
        ],
        compiler_params=pltpu.CompilerParams(
            collective_id=0, has_side_effects=True, vmem_limit_bytes=VMEM_LIMIT
        ),
    )(
        train_query, low_query.T, high_query,
        train_key, low_key.T, high_key,
        train_value, low_value.T, high_value,
        norm_train.reshape(row), norm_step.reshape(row),
    )
    *finals, scale_q, scale_k, scale_v, serve = pl.pallas_call(
        finish,
        name="finish",
        out_shape=(
            *[jax.ShapeDtypeStruct(whole, jnp.bfloat16)] * 3,
            *[jax.ShapeDtypeStruct(row, jnp.float32)] * 3,
            jax.ShapeDtypeStruct(gain, jnp.bfloat16),
        ),
        in_specs=[vmem] * 7,
        out_specs=(anywhere,) * 7,
        scratch_shapes=[
            pltpu.VMEM(whole, jnp.bfloat16), pltpu.VMEM(row, jnp.float32), dma((14,)),
        ],
        compiler_params=pltpu.CompilerParams(vmem_limit_bytes=16 << 20),
    )(*middle)
    return (
        *[final.T for final in finals],
        scale_q.reshape(OWN), scale_k.reshape(OWN), scale_v.reshape(OWN),
        serve.reshape(D_MODEL),
    )


def solution(mesh):
    weights = (P(("site", "zero"), "width"), P(("site", "zero"), None), P("site", "width"))
    gain = P(("site", "zero", "width"))
    return jax.shard_map(
        shards,
        mesh=mesh,
        in_specs=weights * 3 + (gain, gain),
        out_specs=(P("site", ("width", "zero")),) * 3
        + (P(("site", "width", "zero")),) * 3
        + (P("site"),),
        check_vma=False,
    )
```
